32 devices in a mesh: dp: 8 (over z, x), tensor: 4 (over y, core).
Axes of the slice: x: 2, y: 2, z: 4, core: 2. Of those that a mesh axis runs over, the one named last changes fastest.
Arguments:
- tokens: bfloat16 [16, 128, 2048], P('dp'), may hold values from -6 to 6
- cotangent: bfloat16 [16, 128, 2048], P('dp'), may hold values from -6 to 6
- routes: int32 [16, 128, 4], P('dp'), may hold values from 0 to 5, as said below
- gates: bfloat16 [16, 128, 4], P('dp'), may hold values from 0.099609375 to 0.5
- lengths: int32 [16], P('dp'), may hold values from 64 to 128, as said below
- deal: int32 [16], replicated, may hold values from 0 to 15, as said below
- norm1_gain: float32 [2048], P('dp'), may hold values from 0.1 to 1.9
- q_weight: float32 [2048, 2048], P('dp', 'tensor'), may hold values from -0.125 to 0.125
- q_bias: float32 [16, 128], P('tensor', 'dp'), may hold values from -3 to 3
- k_weight: float32 [2048, 2048], P('dp', 'tensor'), may hold values from -0.125 to 0.125
- v_weight: float32 [2048, 2048], P('dp', 'tensor'), may hold values from -0.125 to 0.125
- v_bias: float32 [16, 128], P('tensor', 'dp'), may hold values from -3 to 3
- o_weight: float32 [2048, 2048], P('tensor', 'dp'), may hold values from -0.75 to 0.75
- norm2_gain: float32 [2048], P('dp'), may hold values from 0.1 to 1.9
- expert_gate: float32 [6, 2048, 1408], P(None, 'dp', 'tensor'), may hold values from -0.125 to 0.125
- expert_up: float32 [6, 2048, 1408], P(None, 'dp', 'tensor'), may hold values from -0.125 to 0.125
- expert_down: float32 [6, 1408, 2048], P(None, 'tensor', 'dp'), may hold values from -0.21875 to 0.21875
- shared_gate: float32 [2048, 5632], P('dp', 'tensor'), may hold values from -0.125 to 0.125
- shared_up: float32 [2048, 5632], P('dp', 'tensor'), may hold values from -0.125 to 0.125
- shared_down: float32 [5632, 2048], P('tensor', 'dp'), may hold values from -0.109375 to 0.109375
- shared_switch: float32 [2048], P('dp'), may hold values from -0.125 to 0.125
Outputs:
- output: float32 [16, 128, 2048], P('dp', None, 'tensor')
- tokens_grad: float32 [16, 128, 2048], P('dp', None, 'tensor')
- norm1_gain_grad: float32 [2048], P('dp')
- q_weight_grad: float32 [2048, 2048], P('dp', 'tensor')
- q_bias_grad: float32 [16, 128], P('tensor', 'dp')
- k_weight_grad: float32 [2048, 2048], P('dp', 'tensor')
- v_weight_grad: float32 [2048, 2048], P('dp', 'tensor')
- v_bias_grad: float32 [16, 128], P('tensor', 'dp')
- o_weight_grad: float32 [2048, 2048], P('tensor', 'dp')
- norm2_gain_grad: float32 [2048], P('dp')
- expert_gate_grad: float32 [6, 2048, 1408], P(None, 'dp', 'tensor')
- expert_up_grad: float32 [6, 2048, 1408], P(None, 'dp', 'tensor')
- expert_down_grad: float32 [6, 1408, 2048], P(None, 'tensor', 'dp')
- shared_gate_grad: float32 [2048, 5632], P('dp', 'tensor')
- shared_up_grad: float32 [2048, 5632], P('dp', 'tensor')
- shared_down_grad: float32 [5632, 2048], P('tensor', 'dp')
- shared_switch_grad: float32 [2048], P('dp')
The draws below stay inside these ranges and needn't reach their ends.
Inputs may be any that keep to these rules, and one draw needn't show every extreme that they name: Sequences 2i and 2i+1 are given on dp index i. The two sequences dealt to one dp index have lengths adding up to exactly 192. `deal`: dealt slot 2i holds sequence 2i; the odd sequences move by one common rotation of the dp indices: slot 2i+1 holds sequence 2((i - r) mod the number of dp indices) + 1, for one r of the draw. `routes`: each row names 4 different experts. Among the 192 real tokens dealt to one dp index, every expert is named by exactly 128 tokens. Rows past a sequence's length hold valid ids too.
All inputs are finite; a program needn't handle non-finite values.
Results may differ from the reference program's by a relative error of at most 0.013.
The reference program's roundings to bfloat16 on the way count: a program that leaves them out, or rounds other values in their place, can miss the bound.
Values may be sent and summed in bfloat16 or wider, within the bound.
A program may use at most 256 MiB of HBM per device.

```python
import jax
import jax.numpy as jnp
from jax import lax

D = 2048
HEADS = 16
HEAD_DIM = 128
EXPERT_FF = 1408
SHARED_FF = 5632
EXPERTS = 6
TOP = 4
LMAX = 128
SPAN = 192
SLOTS = 16
N_DP = 8


def deal_plan(key):
    base = jax.random.fold_in(key, 7)
    turn_key, length_key, pick_key = jax.random.split(base, 3)
    rotation = jax.random.randint(turn_key, (), 0, N_DP)
    first_lengths = jax.random.randint(length_key, (N_DP,), LMAX // 2, LMAX + 1)
    chosen = jax.random.randint(pick_key, (), 0, N_DP)
    first_lengths = jnp.where(jnp.arange(N_DP) == chosen, LMAX, first_lengths)
    return (rotation, first_lengths)


def draw_lengths(key, part):
    rotation, first_lengths = deal_plan(key)
    device_ids = jnp.arange(N_DP)
    second_lengths = SPAN - first_lengths[(device_ids + rotation) % N_DP]
    return jnp.stack([first_lengths, second_lengths], axis=1).reshape(-1).astype(jnp.int32)


def draw_deal(key, part):
    rotation, first_lengths = deal_plan(key)
    device_ids = jnp.arange(N_DP)
    sources = 2 * ((device_ids - rotation) % N_DP) + 1
    return jnp.stack([2 * device_ids, sources], axis=1).reshape(-1).astype(jnp.int32)


def draw_routes(key, part):
    rotation, first_lengths = deal_plan(key)
    base = jax.random.fold_in(key, 11)
    rank_key, label_key, filler_key = jax.random.split(base, 3)
    ranks = jax.vmap(lambda subkey: jax.random.permutation(subkey, SPAN))(jax.random.split(rank_key, N_DP))
    labels = jax.vmap(lambda subkey: jax.random.permutation(subkey, EXPERTS))(jax.random.split(label_key, N_DP))
    offsets = jnp.arange(TOP)
    chosen = (ranks[:, :, None] % EXPERTS + offsets) % EXPERTS
    table = jnp.take_along_axis(jnp.broadcast_to(labels[:, None, :], (N_DP, SPAN, EXPERTS)), chosen, axis=2)
    filler_ranks = jax.random.randint(filler_key, (N_DP, 2, LMAX), 0, EXPERTS)
    filler_table = (filler_ranks[..., None] + offsets) % EXPERTS
    places = jnp.arange(LMAX)
    device_ids = jnp.arange(N_DP)
    front_routes = jnp.where((places[None, :] < first_lengths[:, None])[..., None], table[:, :LMAX], filler_table[:, 0])
    receiver = (device_ids + rotation) % N_DP
    back_length = SPAN - first_lengths[receiver]
    back_index = jnp.minimum(first_lengths[receiver][:, None] + places[None, :], SPAN - 1)
    back_table = table[receiver[:, None], back_index]
    back_routes = jnp.where((places[None, :] < back_length[:, None])[..., None], back_table, filler_table[:, 1])
    return jnp.stack([front_routes, back_routes], axis=1).reshape(2 * N_DP, LMAX, TOP).astype(jnp.int32)


def levels(stream_key, dims, shards, low, top_value):
    def one(dim, shards_of):
        steps = jax.random.uniform(jax.random.fold_in(jax.random.fold_in(stream_key, 6), dim), (shards_of,), jnp.float32, low / len(shards), top_value / len(shards))
        return jnp.repeat(jnp.exp(steps), dims[dim] // shards_of).reshape((-1,) + (1,) * (len(dims) - dim - 1))

    loudness = one(*shards[0])
    for cut in shards[1:]:
        loudness = loudness * one(*cut)
    return loudness


def gaussian(own_key, shape, spread, bound, shards=(), kind=jnp.bfloat16):
    entries = spread * jax.random.normal(own_key, shape, jnp.float32)
    if shards:
        entries = entries * levels(own_key, shape, shards, -0.22, 0.18)
    return jnp.clip(entries, -bound, bound).astype(kind)


def setup_inputs(seed: int = 0) -> dict:
    key_of = jax.random.split(jax.random.key(seed), 22)
    tokens = gaussian(key_of[0], (SLOTS, LMAX, D), 1.0, 6.0, ((0, 8),))
    cotangent = gaussian(key_of[1], (SLOTS, LMAX, D), 1.0, 6.0, ((0, 8),))
    routes = draw_routes(jax.random.fold_in(key_of[21], 71), 0)
    gates = jnp.clip(0.099609375 + 0.40039062 * jax.random.uniform(key_of[3], (SLOTS, LMAX, TOP), jnp.float32) ** levels(key_of[3], (SLOTS, LMAX, TOP), ((0, 8),), -0.2, 0.2), 0.099609375, 0.5).astype(jnp.bfloat16)
    lengths = draw_lengths(jax.random.fold_in(key_of[21], 71), 0)
    deal = draw_deal(jax.random.fold_in(key_of[21], 71), 0)
    norm1_gain = jnp.clip(1.0 + 0.18 * jax.random.normal(key_of[6], (D,), jnp.float32), 0.1, 1.9)
    q_weight = gaussian(key_of[7], (D, D), D ** -0.5, 0.125, ((0, 8), (1, 4)), jnp.float32)
    q_bias = gaussian(key_of[8], (HEADS, HEAD_DIM), 0.5, 3.0, ((0, 4), (1, 8)), jnp.float32)
    k_weight = gaussian(key_of[9], (D, D), D ** -0.5, 0.125, ((0, 8), (1, 4)), jnp.float32)
    v_weight = gaussian(key_of[10], (D, D), D ** -0.5, 0.125, ((0, 8), (1, 4)), jnp.float32)
    v_bias = gaussian(key_of[11], (HEADS, HEAD_DIM), 0.5, 3.0, ((0, 4), (1, 8)), jnp.float32)
    o_weight = gaussian(key_of[12], (D, D), (D // 32) ** -0.5, 0.75, ((0, 4), (1, 8)), jnp.float32)
    norm2_gain = jnp.clip(1.0 + 0.18 * jax.random.normal(key_of[13], (D,), jnp.float32), 0.1, 1.9)
    expert_gate = gaussian(key_of[14], (EXPERTS, D, EXPERT_FF), D ** -0.5, 0.125, ((1, 8), (2, 4)), jnp.float32)
    expert_up = gaussian(key_of[15], (EXPERTS, D, EXPERT_FF), D ** -0.5, 0.125, ((1, 8), (2, 4)), jnp.float32)
    expert_down = gaussian(key_of[16], (EXPERTS, EXPERT_FF, D), (EXPERT_FF // 2) ** -0.5, 0.21875, ((1, 4), (2, 8)), jnp.float32)
    shared_gate = gaussian(key_of[17], (D, SHARED_FF), D ** -0.5, 0.125, ((0, 8), (1, 4)), jnp.float32)
    shared_up = gaussian(key_of[18], (D, SHARED_FF), D ** -0.5, 0.125, ((0, 8), (1, 4)), jnp.float32)
    shared_down = gaussian(key_of[19], (SHARED_FF, D), (SHARED_FF // 2) ** -0.5, 0.109375, ((0, 4), (1, 8)), jnp.float32)
    shared_switch = gaussian(key_of[20], (D,), D ** -0.5, 0.125, ((0, 8),), jnp.float32)
    return dict(tokens=tokens, cotangent=cotangent, routes=routes, gates=gates, lengths=lengths, deal=deal, norm1_gain=norm1_gain, q_weight=q_weight, q_bias=q_bias, k_weight=k_weight, v_weight=v_weight, v_bias=v_bias, o_weight=o_weight, norm2_gain=norm2_gain, expert_gate=expert_gate, expert_up=expert_up, expert_down=expert_down, shared_gate=shared_gate, shared_up=shared_up, shared_down=shared_down, shared_switch=shared_switch)


EPSILON = 1e-06
NEGATIVE = -1e+30

@jax.custom_vjp
def low(v):
    return lax.optimization_barrier(v.astype(jnp.bfloat16)).astype(jnp.float32)

@jax.custom_vjp
def low_back(v):
    return v

def low_keep(v):
    return (low(v), None)

def low_pass(kept, grad):
    return (grad,)

def back_keep(v):
    return (v, None)

def back_low(kept, grad):
    return (low(grad),)
low.defvjp(low_keep, low_pass)
low_back.defvjp(back_keep, back_low)

def matmul(left, right):
    return jnp.dot(left, right, precision=lax.Precision.HIGHEST)

def rms_norm(values, gain):
    return values * lax.rsqrt(lax.optimization_barrier(jnp.mean(values * values, axis=-1, keepdims=True)) + EPSILON) * gain

def group_layer(packed, route_rows, gate_rows, first_len, params):
    norm1_gain, q_weight, q_bias, k_weight, v_weight, v_bias, o_weight, norm2_gain, expert_gate, expert_up, expert_down, shared_gate, shared_up, shared_down, shared_switch = [low(weight) for weight in params]
    positions = jnp.arange(SPAN, dtype=jnp.int32)
    second_doc = positions >= first_len
    allowed = (positions[None, :] <= positions[:, None]) & (second_doc[None, :] == second_doc[:, None])
    normed_one = low(rms_norm(packed, norm1_gain))
    queries = low_back(low(matmul(normed_one, q_weight) + q_bias.reshape(-1)))
    key_rows = low_back(low(matmul(normed_one, k_weight)))
    value_rows = low_back(low(matmul(normed_one, v_weight) + v_bias.reshape(-1)))
    head_shape = (SPAN, HEADS, HEAD_DIM)
    scores = jnp.einsum('qhd,khd->hqk', queries.reshape(head_shape), key_rows.reshape(head_shape), precision=lax.Precision.HIGHEST) * HEAD_DIM ** (-0.5)
    scores = low_back(scores)
    scores = jnp.where(allowed[None], scores, NEGATIVE)
    attn_probs = low(jnp.exp(scores - jax.nn.logsumexp(scores, axis=-1, keepdims=True)))
    attended = jnp.einsum('hqk,khd->qhd', attn_probs, value_rows.reshape(head_shape), precision=lax.Precision.HIGHEST).reshape(SPAN, D)
    attended = low_back(low(attended))
    middle = packed + low_back(matmul(attended, o_weight))
    normed_two = low(rms_norm(middle, norm2_gain))
    expert_mix = jnp.zeros_like(middle)
    for expert in range(EXPERTS):
        route_share = lax.optimization_barrier(jnp.sum(jnp.where(route_rows == expert, gate_rows, 0.0), axis=-1))
        gate_act = low_back(matmul(normed_two, expert_gate[expert]))
        up_act = low_back(matmul(normed_two, expert_up[expert]))
        inner_act = low(jax.nn.silu(gate_act) * up_act)
        expert_mix = expert_mix + route_share[:, None] * low_back(matmul(inner_act, expert_down[expert]))
    shared_act = low_back(matmul(normed_two, shared_gate))
    shared_lift = low_back(matmul(normed_two, shared_up))
    shared_inner = low(jax.nn.silu(shared_act) * shared_lift)
    shared_out = low_back(matmul(shared_inner, shared_down))
    switch_gate = jax.nn.sigmoid(matmul(normed_two, shared_switch))
    return middle + expert_mix + switch_gate[:, None] * shared_out

def reference(tokens, cotangent, routes, gates, lengths, deal, norm1_gain, q_weight, q_bias, k_weight, v_weight, v_bias, o_weight, norm2_gain, expert_gate, expert_up, expert_down, shared_gate, shared_up, shared_down, shared_switch):
    groups = jnp.arange(N_DP, dtype=jnp.int32)
    first_seq = deal[2 * groups].astype(jnp.int32)
    second_seq = deal[2 * groups + 1].astype(jnp.int32)
    first_len = lengths[first_seq].astype(jnp.int32)
    positions = jnp.arange(SPAN, dtype=jnp.int32)
    second_doc = positions[None, :] >= first_len[:, None]
    slot_index = jnp.where(second_doc, second_seq[:, None], first_seq[:, None]).astype(jnp.int32)
    row_index = jnp.where(second_doc, positions[None, :] - first_len[:, None], positions[None, :]).astype(jnp.int32)
    packed_routes = routes[slot_index, row_index]
    packed_gates = gates[slot_index, row_index].astype(jnp.float32)
    group_step = jax.checkpoint(group_layer)

    def forward(flat_tokens, params):
        gathered = flat_tokens[slot_index, row_index]

        def one_group(group_items):
            return group_step(group_items[0], group_items[1], group_items[2], group_items[3], params)
        results = lax.map(one_group, (gathered, packed_routes, packed_gates, first_len))
        return jnp.zeros_like(flat_tokens).at[slot_index, row_index].set(results)
    params = (norm1_gain, q_weight, q_bias, k_weight, v_weight, v_bias, o_weight, norm2_gain, expert_gate, expert_up, expert_down, shared_gate, shared_up, shared_down, shared_switch)
    output, pullback = jax.vjp(forward, tokens.astype(jnp.float32), params)
    tokens_grad, weight_grads = pullback(cotangent.astype(jnp.float32))
    return (output, tokens_grad, weight_grads[0], weight_grads[1], weight_grads[2], weight_grads[3], weight_grads[4], weight_grads[5], weight_grads[6], weight_grads[7], weight_grads[8], weight_grads[9], weight_grads[10], weight_grads[11], weight_grads[12], weight_grads[13], weight_grads[14])
```

```python
from functools import partial

import jax
import jax.numpy as jnp
from jax import lax
from jax.sharding import PartitionSpec as P

HEAD_DIM = 128
EPSILON = 1e-06
NEGATIVE = -1e30
LANES = 128
BF16 = jnp.bfloat16
F32 = jnp.float32
ALL = ("dp", "tensor")


def normalize(values, gain):
    return values * lax.rsqrt(jnp.mean(values * values, axis=-1, keepdims=True) + EPSILON) * gain


def nt(left, right):
    return lax.dot_general(left, right, (((1,), (1,)), ((), ())), preferred_element_type=F32)


def tn(left, right):
    return lax.dot_general(left, right, (((0,), (0,)), ((), ())), preferred_element_type=F32)


def nn(left, right):
    return lax.dot_general(left, right, (((1,), (0,)), ((), ())), preferred_element_type=F32)


def gather_all(value):
    return lax.all_gather(value, ALL, axis=0, tiled=True)


def scatter_all(value):
    return lax.psum_scatter(value, ALL, scatter_dimension=0, tiled=True)


def exchange_dp(value):
    return lax.all_to_all(value, "dp", 0, 0, tiled=False)


def per_device(
    tokens,
    cotangent,
    routes,
    gates,
    lengths,
    deal,
    norm1_gain,
    q_weight,
    q_bias,
    k_weight,
    v_weight,
    v_bias,
    o_weight,
    norm2_gain,
    expert_gate,
    expert_up,
    expert_down,
    shared_gate,
    shared_up,
    shared_down,
    shared_switch,
):
    n_dp = lax.axis_size("dp")
    n_tensor = lax.axis_size("tensor")
    place = lax.axis_index("dp")
    member = lax.axis_index("tensor")
    seqs, span, width = tokens.shape
    rows = seqs * span
    shard = rows // n_tensor
    experts, slice_d, expert_cols = expert_gate.shape
    shared_cols = shared_gate.shape[1]
    head_cols = q_weight.shape[1]
    heads = head_cols // HEAD_DIM

    def own_rows(value):
        return lax.dynamic_slice_in_dim(value, member * shard, shard, 0)

    valid = (jnp.arange(span)[None, :] < lengths[:, None]).reshape(rows, 1)
    dense = jnp.zeros((seqs, span, LANES), F32)
    for rank in range(routes.shape[-1]):
        hit = routes[..., rank, None] == jnp.arange(LANES)
        dense = dense + jnp.where(hit, gates[..., rank, None].astype(F32), 0.0)
    dense = dense.reshape(rows, LANES).astype(BF16)
    cot = jnp.where(valid, cotangent.reshape(rows, width), 0).astype(BF16)
    cot_packed = gather_all(own_rows(jnp.concatenate([cot, dense], axis=1)))

    small = jnp.concatenate(
        [norm1_gain, norm2_gain, shared_switch, q_bias.reshape(-1), v_bias.reshape(-1)]
    ).astype(BF16)
    small = lax.all_gather(small[None, :], "dp", axis=0, tiled=True)
    gain_one = small[:, :slice_d].reshape(-1).astype(F32)
    gain_two = small[:, slice_d : 2 * slice_d].reshape(-1).astype(F32)
    switch = small[:, 2 * slice_d : 3 * slice_d].reshape(1, -1)
    piece = q_bias.shape[1]

    def whole_bias(start):
        part = small[:, start : start + heads * piece].reshape(n_dp, heads, piece)
        return part.transpose(1, 0, 2).reshape(-1).astype(F32)

    bias_q = whole_bias(3 * slice_d)
    bias_v = whole_bias(3 * slice_d + heads * piece)
    attn_weights = jnp.concatenate(
        [q_weight.astype(BF16), k_weight.astype(BF16), v_weight.astype(BF16), o_weight.T.astype(BF16)],
        axis=1,
    )
    attn_weights = lax.all_gather(attn_weights, "dp", axis=0, tiled=True)
    weight_qkv = attn_weights[:, : 3 * head_cols]
    weight_o = attn_weights[:, 3 * head_cols :]

    def by_unit(expert_part, shared_part):
        return jnp.concatenate(
            [
                expert_part.astype(BF16).reshape(n_dp, -1, slice_d),
                shared_part.astype(BF16).reshape(n_dp, -1, slice_d),
            ],
            axis=1,
        )

    gate_sent = by_unit(
        expert_gate.astype(BF16).transpose(0, 2, 1).reshape(-1, slice_d), shared_gate.astype(BF16).T
    )
    up_sent = by_unit(
        expert_up.astype(BF16).transpose(0, 2, 1).reshape(-1, slice_d), shared_up.astype(BF16).T
    )
    down_sent = by_unit(expert_down.reshape(-1, slice_d), shared_down)
    arrived = exchange_dp(jnp.stack([gate_sent, up_sent, down_sent], axis=1))
    units = arrived.shape[2]
    routed = experts * expert_cols // n_dp
    arrived = arrived.transpose(1, 2, 0, 3).reshape(3, units, width)
    gate_units, up_units, down_units = arrived[0], arrived[1], arrived[2]

    inputs = tokens.reshape(rows, width).astype(F32)
    inputs_own = own_rows(inputs)
    normed_one = normalize(inputs, gain_one).astype(BF16)
    projected = nn(normed_one, weight_qkv)
    head_shape = (seqs, span, heads, HEAD_DIM)
    queries = (projected[:, :head_cols] + bias_q).astype(BF16).reshape(head_shape)
    keys = projected[:, head_cols : 2 * head_cols].astype(BF16).reshape(head_shape)
    values = (projected[:, 2 * head_cols :] + bias_v).astype(BF16).reshape(head_shape)
    order = jnp.arange(span)
    causal = order[None, :] <= order[:, None]
    scale = HEAD_DIM ** (-0.5)
    scores = jnp.einsum("bqhd,bkhd->bhqk", queries, keys, preferred_element_type=F32) * scale
    scores = jnp.where(causal, scores, NEGATIVE)
    top = jnp.max(scores, axis=-1, keepdims=True)
    powers = jnp.exp(scores - top)
    probs = powers / jnp.sum(powers, axis=-1, keepdims=True)
    probs_low = probs.astype(BF16)
    attended = (
        jnp.einsum("bhqk,bkhd->bqhd", probs_low, values, preferred_element_type=F32)
        .reshape(rows, -1)
        .astype(BF16)
    )
    attn_part = nt(attended, weight_o)
    middle = inputs_own + lax.psum_scatter(attn_part, "tensor", scatter_dimension=0, tiled=True)

    normed_two = gather_all(normalize(middle, gain_two).astype(BF16))
    cot_all = cot_packed[:, :width]
    route_share = cot_packed[:, width : width + LANES]
    unit_expert = (place * routed + jnp.arange(routed)) // expert_cols
    picks = (jnp.arange(LANES)[:, None] == unit_expert[None, :]).astype(BF16)
    gate_logit = nt(normed_two, switch)
    switch_gate = jax.nn.sigmoid(gate_logit)
    share = jnp.concatenate(
        [nn(route_share, picks), jnp.broadcast_to(switch_gate, (switch_gate.shape[0], units - routed))],
        axis=1,
    )
    gate_act = nt(normed_two, gate_units)
    up_act = nt(normed_two, up_units)
    logistic = jax.nn.sigmoid(gate_act)
    silu = gate_act * logistic
    inner = (silu * up_act).astype(BF16).astype(F32)
    inner_share = (inner * share).astype(BF16)
    mixed = nn(inner_share, down_units).astype(BF16)
    mixed = lax.psum_scatter(mixed, "dp", scatter_dimension=0, tiled=True)
    mixed = lax.psum_scatter(mixed, "tensor", scatter_dimension=1, tiled=True)

    grad_inner_raw = nt(cot_all, down_units)
    grad_logit = (
        jnp.sum(inner[:, routed:] * grad_inner_raw[:, routed:], axis=1, keepdims=True)
        * switch_gate
        * (1.0 - switch_gate)
    )
    grad_inner = grad_inner_raw * share
    slope = logistic * (1.0 + gate_act * (1.0 - logistic))
    grad_gate_act = (grad_inner * up_act * slope).astype(BF16)
    grad_up_act = (grad_inner * silu).astype(BF16)
    back_two = nn(grad_gate_act, gate_units) + nn(grad_up_act, up_units)
    back_two = (back_two + grad_logit * switch.astype(F32)).astype(BF16)
    back_two = scatter_all(back_two).astype(F32)
    grad_down = tn(inner_share, cot_all)
    grad_gate = tn(grad_gate_act, normed_two)
    grad_up = tn(grad_up_act, normed_two)
    grad_switch = jnp.sum(grad_logit * normed_two.astype(F32), axis=0)
    sent_back = jnp.stack([grad_gate, grad_up, grad_down]).astype(BF16)
    sent_back = sent_back.reshape(3, units, n_dp, slice_d).transpose(2, 0, 1, 3)
    returned = exchange_dp(sent_back).astype(F32)

    def split_units(value):
        routed_part = value[:, :routed].reshape(experts, expert_cols, slice_d)
        return routed_part, value[:, routed:].reshape(shared_cols, slice_d)

    grad_gate_experts, grad_gate_shared = split_units(returned[:, 0])
    grad_up_experts, grad_up_shared = split_units(returned[:, 1])
    grad_down_experts, grad_down_shared = split_units(returned[:, 2])

    unused_two, norm_two_back = jax.vjp(normalize, middle, gain_two)
    grad_middle_norm, grad_gain_two = norm_two_back(back_two)
    grad_middle = own_rows(cot).astype(F32) + grad_middle_norm
    grad_attn = lax.all_gather(grad_middle.astype(BF16), "tensor", axis=0, tiled=True)
    grad_weight_o = tn(grad_attn, attended)
    grad_attended = nn(grad_attn, weight_o).astype(BF16).reshape(head_shape)
    grad_values = (
        jnp.einsum("bhqk,bqhd->bkhd", probs_low, grad_attended, preferred_element_type=F32)
        .astype(BF16)
        .reshape(rows, -1)
    )
    grad_probs = jnp.einsum("bqhd,bkhd->bhqk", grad_attended, values, preferred_element_type=F32)
    grad_scores = (
        probs * (grad_probs - jnp.sum(grad_probs * probs, axis=-1, keepdims=True))
    ).astype(BF16)
    grad_queries = (
        (jnp.einsum("bhqk,bkhd->bqhd", grad_scores, keys, preferred_element_type=F32) * scale)
        .astype(BF16)
        .reshape(rows, -1)
    )
    grad_keys = (
        (jnp.einsum("bhqk,bqhd->bkhd", grad_scores, queries, preferred_element_type=F32) * scale)
        .astype(BF16)
        .reshape(rows, -1)
    )
    grad_qkv = jnp.concatenate([grad_queries, grad_keys, grad_values], axis=1)
    grad_attn_weights = jnp.concatenate([tn(normed_one, grad_qkv), grad_weight_o], axis=1).astype(BF16)
    grad_attn_weights = lax.psum_scatter(
        grad_attn_weights, "dp", scatter_dimension=0, tiled=True
    ).astype(F32)
    back_one = nt(grad_qkv, weight_qkv)
    back_one = lax.psum_scatter(back_one, "tensor", scatter_dimension=0, tiled=True)
    unused_one, norm_one_back = jax.vjp(normalize, inputs_own, gain_one)
    grad_input_norm, grad_gain_one = norm_one_back(back_one)
    grad_input = grad_middle + grad_input_norm

    bias_part = jnp.concatenate(
        [
            jnp.sum(grad_queries.astype(F32), axis=0).reshape(heads, n_dp, piece),
            jnp.sum(grad_values.astype(F32), axis=0).reshape(heads, n_dp, piece),
        ],
        axis=0,
    )
    bias_part = bias_part.transpose(1, 0, 2).reshape(1, n_dp, -1)
    mine = (jnp.arange(n_tensor) == member)[:, None, None]
    bias_part = jnp.where(mine, bias_part, 0.0)
    gains = jnp.concatenate([grad_gain_one, grad_gain_two, grad_switch])
    gains = gains.reshape(1, 3, n_dp, slice_d).transpose(0, 2, 1, 3).reshape(n_dp, 3 * slice_d)
    pack = jnp.concatenate([gains, bias_part.transpose(1, 0, 2).reshape(n_dp, -1)], axis=1)
    pack = lax.psum(pack, ALL)
    pack = lax.dynamic_slice_in_dim(pack, place, 1, 0)[0]
    bias_own = lax.dynamic_slice_in_dim(
        pack[3 * slice_d :].reshape(n_tensor, 2, heads, piece), member, 1, 0
    )[0]

    def to_columns(value):
        return lax.all_to_all(value, "tensor", 1, 0, tiled=True)

    out_shape = (seqs, span, width // n_tensor)
    output = jnp.where(valid, to_columns(middle) + mixed.astype(F32), 0.0).reshape(out_shape)
    tokens_grad = jnp.where(valid, to_columns(grad_input), 0.0).reshape(out_shape)
    return (
        output,
        tokens_grad,
        pack[:slice_d],
        grad_attn_weights[:, :head_cols],
        bias_own[0],
        grad_attn_weights[:, head_cols : 2 * head_cols],
        grad_attn_weights[:, 2 * head_cols : 3 * head_cols],
        bias_own[1],
        grad_attn_weights[:, 3 * head_cols :].T,
        pack[slice_d : 2 * slice_d],
        grad_gate_experts.transpose(0, 2, 1),
        grad_up_experts.transpose(0, 2, 1),
        grad_down_experts,
        grad_gate_shared.T,
        grad_up_shared.T,
        grad_down_shared,
        pack[2 * slice_d : 3 * slice_d],
    )


IN_SPECS = (
    P("dp", None, None),
    P("dp", None, None),
    P("dp", None, None),
    P("dp", None, None),
    P("dp"),
    P(),
    P("dp"),
    P("dp", "tensor"),
    P("tensor", "dp"),
    P("dp", "tensor"),
    P("dp", "tensor"),
    P("tensor", "dp"),
    P("tensor", "dp"),
    P("dp"),
    P(None, "dp", "tensor"),
    P(None, "dp", "tensor"),
    P(None, "tensor", "dp"),
    P("dp", "tensor"),
    P("dp", "tensor"),
    P("tensor", "dp"),
    P("dp"),
)
OUT_SPECS = (P("dp", None, "tensor"), P("dp", None, "tensor")) + IN_SPECS[6:]


def solution(mesh):
    return jax.shard_map(
        per_device, mesh=mesh, in_specs=IN_SPECS, out_specs=OUT_SPECS, check_vma=False
    )
```

```python
import jax
import jax.numpy as jnp
from jax import lax
from jax.sharding import PartitionSpec as P


HEAD_DIM = 128
EPSILON = 1e-06
NEGATIVE = -1e30
LANES = 128
BF16 = jnp.bfloat16
F32 = jnp.float32
ALL = ("dp", "tensor")


def normalize(values, gain):
    return values * lax.rsqrt(jnp.mean(values * values, axis=-1, keepdims=True) + EPSILON) * gain


def nt(left, right):
    return lax.dot_general(left, right, (((1,), (1,)), ((), ())), preferred_element_type=F32)


def tn(left, right):
    return lax.dot_general(left, right, (((0,), (0,)), ((), ())), preferred_element_type=F32)


def nn(left, right):
    return lax.dot_general(left, right, (((1,), (0,)), ((), ())), preferred_element_type=F32)


def gather_all(value):
    return lax.all_gather(value, ALL, axis=0, tiled=True)


def swap(value, axis, bit):
    count = lax.axis_size(axis)
    pairs = [(source, source ^ (1 << bit)) for source in range(count)]
    return lax.ppermute(value, axis, pairs)


def bits_of(axis):
    return [(axis, bit) for bit in range(lax.axis_size(axis).bit_length() - 1)]


def link_orders():
    tensor_bits = bits_of("tensor")
    dp_bits = bits_of("dp")
    first, rest = tensor_bits[:1], tensor_bits[1:]
    return (first + rest + dp_bits, first + dp_bits + rest)


def halving(value, order):
    dims = bits_of("dp")[::-1] + bits_of("tensor")[::-1]
    width = value.shape[-1]
    value = value.reshape((2,) * len(dims) + (-1, width))
    for axis, bit in order:
        dim = dims.index((axis, bit))
        mine = (lax.axis_index(axis) >> bit) & 1
        kept = lax.dynamic_index_in_dim(value, mine, dim)
        sent = lax.dynamic_index_in_dim(value, 1 - mine, dim)
        value = (kept.astype(F32) + swap(sent, axis, bit).astype(F32)).astype(BF16)
    return value.reshape(-1, width)


def scatter_all(parts):
    return jnp.concatenate(
        [halving(part, order) for part, order in zip(parts, link_orders())], axis=1
    )


def exchange_dp(value):
    return lax.all_to_all(value, "dp", 0, 0, tiled=False)


def layer(
    tokens,
    cotangent,
    routes,
    gates,
    lengths,
    deal,
    norm1_gain,
    q_weight,
    q_bias,
    k_weight,
    v_weight,
    v_bias,
    o_weight,
    norm2_gain,
    expert_gate,
    expert_up,
    expert_down,
    shared_gate,
    shared_up,
    shared_down,
    shared_switch,
):
    n_dp = lax.axis_size("dp")
    n_tensor = lax.axis_size("tensor")
    place = lax.axis_index("dp")
    member = lax.axis_index("tensor")
    seqs, span, width = tokens.shape
    rows = seqs * span
    shard = rows // n_tensor
    experts, slice_d, expert_cols = expert_gate.shape
    shared_cols = shared_gate.shape[1]
    head_cols = q_weight.shape[1]
    heads = head_cols // HEAD_DIM

    def own_rows(value):
        return lax.dynamic_slice_in_dim(value, member * shard, shard, 0)

    valid = (jnp.arange(span)[None, :] < lengths[:, None]).reshape(rows, 1)
    dense = jnp.zeros((seqs, span, LANES), F32)
    for rank in range(routes.shape[-1]):
        hit = routes[..., rank, None] == jnp.arange(LANES)
        dense = dense + jnp.where(hit, gates[..., rank, None].astype(F32), 0.0)
    dense = dense.reshape(rows, LANES).astype(BF16)
    cot = jnp.where(valid, cotangent.reshape(rows, width), 0).astype(BF16)
    cot_own = own_rows(jnp.concatenate([cot, dense], axis=1))
    cot_packed = gather_all(cot_own)

    small = jnp.concatenate(
        [norm1_gain, norm2_gain, shared_switch, q_bias.reshape(-1), v_bias.reshape(-1)]
    ).astype(BF16)
    small = lax.all_gather(small[None, :], "dp", axis=0, tiled=True)
    gain_one = small[:, :slice_d].reshape(-1).astype(F32)
    gain_two = small[:, slice_d : 2 * slice_d].reshape(-1).astype(F32)
    switch = small[:, 2 * slice_d : 3 * slice_d].reshape(1, -1)
    piece = q_bias.shape[1]

    def whole_bias(start):
        part = small[:, start : start + heads * piece].reshape(n_dp, heads, piece)
        return part.transpose(1, 0, 2).reshape(-1).astype(F32)

    bias_q = whole_bias(3 * slice_d)
    bias_v = whole_bias(3 * slice_d + heads * piece)
    attn_weights = jnp.concatenate(
        [q_weight.astype(BF16), k_weight.astype(BF16), v_weight.astype(BF16), o_weight.T.astype(BF16)],
        axis=1,
    )
    attn_weights = lax.all_gather(attn_weights, "dp", axis=0, tiled=True)
    weight_qkv = attn_weights[:, : 3 * head_cols]
    weight_o = attn_weights[:, 3 * head_cols :]

    def by_unit(expert_part, shared_part):
        return jnp.concatenate(
            [
                expert_part.astype(BF16).reshape(n_dp, -1, slice_d),
                shared_part.astype(BF16).reshape(n_dp, -1, slice_d),
            ],
            axis=1,
        )

    gate_sent = by_unit(
        expert_gate.astype(BF16).transpose(0, 2, 1).reshape(-1, slice_d), shared_gate.astype(BF16).T
    )
    up_sent = by_unit(
        expert_up.astype(BF16).transpose(0, 2, 1).reshape(-1, slice_d), shared_up.astype(BF16).T
    )
    down_sent = by_unit(expert_down.reshape(-1, slice_d), shared_down)
    units_sent = jnp.stack([gate_sent, up_sent, down_sent], axis=1)
    arrived = exchange_dp(units_sent)
    units = arrived.shape[2]
    routed = experts * expert_cols // n_dp
    arrived = arrived.transpose(1, 2, 0, 3).reshape(3, units, width)
    gate_units, up_units, down_units = arrived[0], arrived[1], arrived[2]

    inputs = tokens.reshape(rows, width).astype(F32)
    inputs_own = own_rows(inputs)
    normed_one = normalize(inputs, gain_one).astype(BF16)
    projected = nn(normed_one, weight_qkv)
    head_shape = (seqs, span, heads, HEAD_DIM)
    queries = (projected[:, :head_cols] + bias_q).astype(BF16).reshape(head_shape)
    keys = projected[:, head_cols : 2 * head_cols].astype(BF16).reshape(head_shape)
    values = (projected[:, 2 * head_cols :] + bias_v).astype(BF16).reshape(head_shape)
    order = jnp.arange(span)
    causal = order[None, :] <= order[:, None]
    scale = HEAD_DIM ** (-0.5)
    scores = jnp.einsum("bqhd,bkhd->bhqk", queries, keys, preferred_element_type=F32) * scale
    scores = jnp.where(causal, scores, NEGATIVE)
    top = jnp.max(scores, axis=-1, keepdims=True)
    powers = jnp.exp(scores - top)
    probs = powers / jnp.sum(powers, axis=-1, keepdims=True)
    probs_low = probs.astype(BF16)
    attended = (
        jnp.einsum("bhqk,bkhd->bqhd", probs_low, values, preferred_element_type=F32)
        .reshape(rows, -1)
        .astype(BF16)
    )
    attn_part = nt(attended, weight_o)
    middle = inputs_own + lax.psum_scatter(attn_part, "tensor", scatter_dimension=0, tiled=True)

    normed_two = gather_all(normalize(middle, gain_two).astype(BF16))
    cot_all = cot_packed[:, :width]
    route_share = cot_packed[:, width : width + LANES]
    unit_expert = (place * routed + jnp.arange(routed)) // expert_cols
    picks = (jnp.arange(LANES)[:, None] == unit_expert[None, :]).astype(BF16)
    gate_logit = nt(normed_two, switch)
    switch_gate = jax.nn.sigmoid(gate_logit)
    share = jnp.concatenate(
        [nn(route_share, picks), jnp.broadcast_to(switch_gate, (switch_gate.shape[0], units - routed))],
        axis=1,
    )
    gate_act = nt(normed_two, gate_units)
    up_act = nt(normed_two, up_units)
    logistic = jax.nn.sigmoid(gate_act)
    silu = gate_act * logistic
    inner = (silu * up_act).astype(BF16).astype(F32)
    inner_share = (inner * share).astype(BF16)
    half = width // 2
    mixed = scatter_all(
        [nn(inner_share, down_units[:, cut : cut + half]).astype(BF16) for cut in (0, half)]
    )

    grad_inner_raw = nt(cot_all, down_units)
    grad_logit = (
        jnp.sum(inner[:, routed:] * grad_inner_raw[:, routed:], axis=1, keepdims=True)
        * switch_gate
        * (1.0 - switch_gate)
    )
    grad_inner = grad_inner_raw * share
    slope = logistic * (1.0 + gate_act * (1.0 - logistic))
    grad_gate_act = (grad_inner * up_act * slope).astype(BF16)
    grad_up_act = (grad_inner * silu).astype(BF16)
    both_acts = jnp.concatenate([grad_gate_act, grad_up_act], axis=1)
    both_units = jnp.concatenate([gate_units, up_units], axis=0)
    back_parts = [
        (
            nn(both_acts, both_units[:, cut : cut + half])
            + grad_logit * switch[:, cut : cut + half].astype(F32)
        ).astype(BF16)
        for cut in (0, half)
    ]
    grad_down = tn(inner_share, cot_all)
    grad_gate = tn(grad_gate_act, normed_two)
    grad_up = tn(grad_up_act, normed_two)
    grad_switch = jnp.sum(grad_logit * normed_two.astype(F32), axis=0)
    sent_back = jnp.stack([grad_gate, grad_up, grad_down]).astype(BF16)
    sent_back = sent_back.reshape(3, units, n_dp, slice_d).transpose(2, 0, 1, 3)
    sent_back, *back_parts = lax.optimization_barrier((sent_back, *back_parts))
    returned = exchange_dp(sent_back)
    returned = returned.astype(F32)
    back_two = scatter_all(back_parts)
    back_two = back_two.astype(F32)

    def split_units(value):
        routed_part = value[:, :routed].reshape(experts, expert_cols, slice_d)
        return routed_part, value[:, routed:].reshape(shared_cols, slice_d)

    grad_gate_experts, grad_gate_shared = split_units(returned[:, 0])
    grad_up_experts, grad_up_shared = split_units(returned[:, 1])
    grad_down_experts, grad_down_shared = split_units(returned[:, 2])

    _, norm_two_back = jax.vjp(normalize, middle, gain_two)
    grad_middle_norm, grad_gain_two = norm_two_back(back_two)
    grad_middle = own_rows(cot).astype(F32) + grad_middle_norm
    grad_attn = lax.all_gather(grad_middle.astype(BF16), "tensor", axis=0, tiled=True)
    grad_weight_o = tn(grad_attn, attended)
    grad_attended = nn(grad_attn, weight_o).astype(BF16).reshape(head_shape)
    grad_values = (
        jnp.einsum("bhqk,bqhd->bkhd", probs_low, grad_attended, preferred_element_type=F32)
        .astype(BF16)
        .reshape(rows, -1)
    )
    grad_probs = jnp.einsum("bqhd,bkhd->bhqk", grad_attended, values, preferred_element_type=F32)
    grad_scores = (
        probs * (grad_probs - jnp.sum(grad_probs * probs, axis=-1, keepdims=True))
    ).astype(BF16)
    grad_queries = (
        (jnp.einsum("bhqk,bkhd->bqhd", grad_scores, keys, preferred_element_type=F32) * scale)
        .astype(BF16)
        .reshape(rows, -1)
    )
    grad_keys = (
        (jnp.einsum("bhqk,bqhd->bkhd", grad_scores, queries, preferred_element_type=F32) * scale)
        .astype(BF16)
        .reshape(rows, -1)
    )
    grad_qkv = jnp.concatenate([grad_queries, grad_keys, grad_values], axis=1)
    grad_attn_weights = jnp.concatenate([tn(normed_one, grad_qkv), grad_weight_o], axis=1).astype(BF16)
    grad_attn_weights = lax.psum_scatter(
        grad_attn_weights, "dp", scatter_dimension=0, tiled=True
    ).astype(F32)
    back_one = nt(grad_qkv, weight_qkv)
    back_one = lax.psum_scatter(back_one, "tensor", scatter_dimension=0, tiled=True)
    _, norm_one_back = jax.vjp(normalize, inputs_own, gain_one)
    grad_input_norm, grad_gain_one = norm_one_back(back_one)
    grad_input = grad_middle + grad_input_norm

    bias_part = jnp.concatenate(
        [
            jnp.sum(grad_queries.astype(F32), axis=0).reshape(heads, n_dp, piece),
            jnp.sum(grad_values.astype(F32), axis=0).reshape(heads, n_dp, piece),
        ],
        axis=0,
    )
    bias_part = bias_part.transpose(1, 0, 2).reshape(1, n_dp, -1)
    mine = (jnp.arange(n_tensor) == member)[:, None, None]
    bias_part = jnp.where(mine, bias_part, 0.0)
    gains = jnp.concatenate([grad_gain_one, grad_gain_two, grad_switch])
    gains = gains.reshape(1, 3, n_dp, slice_d).transpose(0, 2, 1, 3).reshape(n_dp, 3 * slice_d)
    pack = jnp.concatenate([gains, bias_part.transpose(1, 0, 2).reshape(n_dp, -1)], axis=1)
    pack = lax.psum(pack, ALL)
    pack = lax.dynamic_slice_in_dim(pack, place, 1, 0)[0]
    bias_own = lax.dynamic_slice_in_dim(
        pack[3 * slice_d :].reshape(n_tensor, 2, heads, piece), member, 1, 0
    )[0]

    def to_columns(value):
        return lax.all_to_all(value, "tensor", 1, 0, tiled=True)

    out_shape = (seqs, span, width // n_tensor)
    output = jnp.where(valid, to_columns(middle + mixed.astype(F32)), 0.0).reshape(out_shape)
    tokens_grad = jnp.where(valid, to_columns(grad_input), 0.0).reshape(out_shape)
    return (
        output,
        tokens_grad,
        pack[:slice_d],
        grad_attn_weights[:, :head_cols],
        bias_own[0],
        grad_attn_weights[:, head_cols : 2 * head_cols],
        grad_attn_weights[:, 2 * head_cols : 3 * head_cols],
        bias_own[1],
        grad_attn_weights[:, 3 * head_cols :].T,
        pack[slice_d : 2 * slice_d],
        grad_gate_experts.transpose(0, 2, 1),
        grad_up_experts.transpose(0, 2, 1),
        grad_down_experts,
        grad_gate_shared.T,
        grad_up_shared.T,
        grad_down_shared,
        pack[2 * slice_d : 3 * slice_d],
    )


IN_SPECS = (
    P("dp", None, None),
    P("dp", None, None),
    P("dp", None, None),
    P("dp", None, None),
    P("dp"),
    P(),
    P("dp"),
    P("dp", "tensor"),
    P("tensor", "dp"),
    P("dp", "tensor"),
    P("dp", "tensor"),
    P("tensor", "dp"),
    P("tensor", "dp"),
    P("dp"),
    P(None, "dp", "tensor"),
    P(None, "dp", "tensor"),
    P(None, "tensor", "dp"),
    P("dp", "tensor"),
    P("dp", "tensor"),
    P("tensor", "dp"),
    P("dp"),
)
OUT_SPECS = (P("dp", None, "tensor"), P("dp", None, "tensor")) + IN_SPECS[6:]


def solution(mesh):
    return jax.shard_map(layer, mesh=mesh, in_specs=IN_SPECS, out_specs=OUT_SPECS, check_vma=False)
```
